32 devices in a mesh: grp: 4 (over y, x), clu: 8 (over z, core).
Axes of the slice: x: 2, y: 2, z: 4, core: 2. Of those that a mesh axis runs over, the one named last changes fastest.
Arguments:
- forces: bfloat16 [3, 2048, 512], P(None, 'clu'), may hold values from -6 to 6
- order: int32 [2048], P('clu'), may hold values from 0 to 2047, as said below
- bases: bfloat16 [2, 32, 3, 2048], P(None, None, None, 'clu'), may hold values from -0.21875 to 0.21875
- near_tiles: bfloat16 [8, 8, 768, 768], P('clu', 'grp'), may hold values from -0.078125 to 0.078125
- near_col: int32 [8, 8], P('clu', 'grp'), may hold values from 0 to 7, as said below
- far_basis: bfloat16 [8, 64, 32, 768], P('clu', 'grp'), may hold values from -0.125 to 0.125
- far_coupling: bfloat16 [8, 64, 32, 32], P('clu', 'grp'), may hold values from -1 to 1
- far_scale: float32 [8, 64], P('clu', 'grp'), may hold values from 0.5 to 2
- far_rank: int32 [8, 64], P('clu', 'grp'), may hold values from 8 to 32
- far_target: int32 [8, 64], P('clu', 'grp'), may hold values from 0 to 5, as said below
Outputs:
- velocity: float32 [3, 2048, 512], P(None, 'clu', 'grp')
The draws below stay inside these ranges and needn't reach their ends.
Inputs may be any that keep to these rules, and one draw needn't show every extreme that they name: `order`: A permutation of the bead numbers; the 256 positions of row block c hold beads of chain blocks c - 1, c and c + 1 only, counted cyclically, exactly 64 of them from chain block c - 1 and exactly 64 from chain block c + 1. `near_col`: each near tile's column block lies within two blocks of its row block, counted cyclically. `far_target`: level l takes indices 2 ** (l + 1) - 2 to 2 ** (l + 2) - 3; the named cluster never contains the block's own row block.
All inputs are finite; a program needn't handle non-finite values.
Results may differ from the reference program's by a relative error of at most 0.0025.
Values may be sent and summed in bfloat16 or wider, within the bound.
A program may use at most 64 MiB of HBM per device.

```python
import math
import jax
import jax.numpy as jnp
from jax import lax

TILE = 256
RANK = 32
LEVELS = 2
NRHS = 512
FAR_DEV = 16
N_BEADS = 2048
NEARS = 8
FARS = 64
N_CLU = 8


def draw_order(key, part):
    clusters = N_BEADS // TILE
    quarter = TILE // 4
    first_key, second_key = jax.random.split(jax.random.fold_in(key, 11))
    chain_perm = jax.vmap(lambda k: jax.random.permutation(k, TILE))(jax.random.split(first_key, clusters))
    beads = (chain_perm + jnp.arange(clusters)[:, None] * TILE).astype(jnp.int32)
    to_left = beads[:, :quarter]
    to_right = beads[:, quarter:2 * quarter]
    staying = beads[:, 2 * quarter:]
    grouped = jnp.concatenate([staying, jnp.roll(to_left, -1, axis=0), jnp.roll(to_right, 1, axis=0)], axis=1)
    shuffle = jax.vmap(lambda k: jax.random.permutation(k, TILE))(jax.random.split(second_key, clusters))
    grouped = jnp.take_along_axis(grouped, shuffle, axis=1)
    return grouped.reshape(-1).astype(jnp.int32)


def draw_near_col(key, part):
    clusters = N_BEADS // TILE
    offsets = jax.random.randint(jax.random.fold_in(key, 23), (clusters, NEARS), -2, 3)
    rows = jnp.arange(clusters, dtype=jnp.int32)[:, None]
    return jnp.mod(rows + offsets, clusters).astype(jnp.int32)


def draw_far_target(key, part):
    clusters = N_BEADS // TILE
    level_key, step_key = jax.random.split(jax.random.fold_in(key, 37))
    level = jax.random.randint(level_key, (clusters, FARS), 0, LEVELS)
    count = jnp.left_shift(jnp.full((clusters, FARS), 2, jnp.int32), level.astype(jnp.int32))
    members = clusters // count
    rows = jnp.arange(clusters, dtype=jnp.int32)[:, None]
    own = rows // members
    step = jax.random.randint(step_key, (clusters, FARS), 0, count - 1)
    target = jnp.mod(own + 1 + step, count)
    return (count - 2 + target).astype(jnp.int32)


def place_ends(result, own_key, smallest, largest):
    dims = result.shape
    spot = [jax.random.randint(jax.random.fold_in(own_key, axis), (), 0, dims[axis]) for axis in range(len(dims))]
    result = result.at[tuple(spot)].set(smallest)
    longest = dims.index(max(dims))
    spot[longest] = (spot[longest] + 1) % dims[longest]
    return result.at[tuple(spot)].set(largest)


def shard_levels(stream_key, extent, cuts, least, top_value):
    factor_of, own = 1.0, jax.random.fold_in(stream_key, 6)
    for axis_at, parts in cuts:
        steps = jnp.exp(jax.random.uniform(jax.random.fold_in(own, axis_at), (parts,), jnp.float32, least / len(cuts), top_value / len(cuts)))
        factor_of = factor_of * jnp.repeat(steps, extent[axis_at] // parts).reshape([-1 if axis == axis_at else 1 for axis in range(len(extent))])
    return factor_of


def gaussian(own_key, extent, width, reach, cuts=(), held_as=jnp.bfloat16):
    drawn = width * jax.random.normal(own_key, extent, jnp.float32)
    if cuts:
        drawn = drawn * shard_levels(own_key, extent, cuts, -0.22, 0.18)
    return jnp.clip(drawn, -reach, reach).astype(held_as)


def setup_inputs(seed: int = 0) -> dict:
    keys = jax.random.split(jax.random.key(seed), 11)
    return {
        "forces": gaussian(keys[0], (3, N_BEADS, NRHS), 1.0, 6.0, ((1, 8),)),
        "order": draw_order(jax.random.fold_in(keys[10], 71), 0),
        "bases": gaussian(keys[2], (LEVELS, RANK, 3, N_BEADS), (3 * TILE) ** -0.5, 0.21875, ((3, 8),)),
        "near_tiles": gaussian(keys[3], (N_CLU, NEARS, 3 * TILE, 3 * TILE), (3 * TILE * NEARS) ** -0.5, 0.078125, ((0, 8), (1, 4))),
        "near_col": draw_near_col(jax.random.fold_in(keys[10], 71), 0),
        "far_basis": gaussian(keys[5], (N_CLU, FARS, RANK, 3 * TILE), (FAR_DEV * RANK * N_CLU // 2) ** -0.5, 0.125, ((0, 8), (1, 4))),
        "far_coupling": gaussian(keys[6], (N_CLU, FARS, RANK, RANK), RANK ** -0.5, 1.0, ((0, 8), (1, 4))),
        "far_scale": jnp.clip(jnp.exp(math.log(2.0) - 1.3862944 * jax.random.uniform(keys[7], (N_CLU, FARS), jnp.float32) ** shard_levels(keys[7], (N_CLU, FARS), ((0, 8), (1, 4)), -0.2, 0.2)), 0.5, 2.0),
        "far_rank": place_ends(jax.random.randint(keys[8], (N_CLU, FARS), 8, RANK + 1), jax.random.fold_in(keys[8], 1), 8, RANK).astype(jnp.int32),
        "far_target": draw_far_target(jax.random.fold_in(keys[10], 71), 0),
    }


def reference(forces, order, bases, near_tiles, near_col, far_basis, far_coupling, far_scale, far_rank, far_target):
    clusters = N_BEADS // TILE
    clustered = jnp.take(forces, order, axis=1)
    blocks = clustered.reshape(3, clusters, TILE, NRHS).transpose(1, 0, 2, 3).reshape(clusters, 3 * TILE, NRHS)
    basis_blocks = bases.reshape(LEVELS, RANK, 3, clusters, TILE).transpose(3, 0, 1, 2, 4).reshape(clusters, LEVELS * RANK, 3 * TILE)

    def piece_of(pair):
        return jnp.dot(pair[0], pair[1], preferred_element_type=jnp.float32)

    pieces = lax.map(piece_of, (basis_blocks, blocks)).reshape(clusters, LEVELS, RANK, NRHS)
    levels_list = []
    for level in range(LEVELS):
        count = 2 ** (level + 1)
        levels_list.append(pieces[:, level].reshape(count, clusters // count, RANK, NRHS).sum(axis=1))
    table = jnp.concatenate(levels_list, axis=0)

    def row(index):
        columns = near_col[index]
        total = jnp.zeros((3 * TILE, NRHS), jnp.float32)
        for slot in range(NEARS):
            total = total + jnp.dot(near_tiles[index, slot], blocks[columns[slot]], preferred_element_type=jnp.float32)
        picked = table[far_target[index]]
        keep = (jnp.arange(RANK, dtype=jnp.int32)[None, :] < far_rank[index][:, None]).astype(jnp.float32)
        masked = picked * keep[:, :, None]
        coupled = jnp.einsum("brs,bsn->brn", far_coupling[index].astype(jnp.float32), masked, precision=lax.Precision.HIGHEST)
        coupled = (coupled * far_scale[index][:, None, None]).astype(jnp.bfloat16)
        far = lax.dot_general(far_basis[index].reshape(FARS * RANK, 3 * TILE), coupled.reshape(FARS * RANK, NRHS), (((0,), (0,)), ((), ())), preferred_element_type=jnp.float32)
        return total + far

    rows = lax.map(row, jnp.arange(clusters, dtype=jnp.int32))
    return rows.reshape(clusters, 3, TILE, NRHS).transpose(1, 0, 2, 3).reshape(3, N_BEADS, NRHS)
```

```python
import functools

import jax
import jax.numpy as jnp
from jax import lax
from jax.experimental import pallas as pl
from jax.experimental.pallas import tpu as pltpu
from jax.sharding import PartitionSpec as P

MESH = pl.DeviceIdType.MESH
F32, BF16 = jnp.float32, jnp.bfloat16


def kernel(
    n, groups, levels, rank,
    forces, order, bases, tiles_hbm, near_col, basis_hbm, coupling, scale, ranks, targets,
    out,
    raw, ext, ext_out, orders, tiles, basis, spread, picks, own_pick, piece_out, pieces,
    table_out, tables, coupled, total, y_out, y_in,
    local_sem, order_send, order_recv, raw_send, raw_recv, ext_send, ext_recv,
    piece_send, piece_recv, table_send, table_recv, y_send, y_recv,
):
    g, c = lax.axis_index("grp"), lax.axis_index("clu")
    core = lax.rem(c, 2)
    comps, tile, columns = forces.shape
    width = columns // groups
    quarter = tile // 4
    slots = raw.shape[1]
    rows = comps * tile
    near_count = tiles.shape[0]
    far_count = targets.shape[1]
    coarse = 2 ** (levels + 1) - 2

    def at_clu(by):
        return {"grp": g, "clu": lax.rem(c + by + n, n)}

    def at_grp(by):
        return {"grp": lax.rem(g + by, groups), "clu": c}

    mate = {"grp": g, "clu": c + 1 - 2 * core}

    def remote(src, dst, send, recv, where):
        return pltpu.make_async_remote_copy(
            src_ref=src, dst_ref=dst, send_sem=send, recv_sem=recv, device_id=where, device_id_type=MESH
        )

    def own_columns(i):
        q = lax.rem(g + i, groups)
        return forces.at[:, :, pl.ds(pl.multiple_of(q * width, width), width)]

    local = [pltpu.make_async_copy(own_columns(i), raw.at[i, 2 + core], local_sem.at[i]) for i in range(groups)]
    for copy in local:
        copy.start()
    tiles_copy = pltpu.make_async_copy(tiles_hbm, tiles, local_sem.at[groups])
    basis_copy = pltpu.make_async_copy(basis_hbm, basis, local_sem.at[groups + 1])
    tiles_copy.start()
    basis_copy.start()

    barrier = pltpu.get_barrier_semaphore()

    def greet(d, carry):
        pl.semaphore_signal(barrier, inc=1, device_id=at_clu(d), device_id_type=MESH)
        return carry

    lax.fori_loop(1, n, greet, 0)
    for d in range(1, groups):
        pl.semaphore_signal(barrier, inc=1, device_id=at_grp(d), device_id_type=MESH)
    pl.semaphore_wait(barrier, n - 1 + groups - 1)

    sends = []
    offsets = (-2, -1, 1, 2)
    order_copies = []
    for at, by in enumerate(offsets):
        copy = remote(order, orders.at[2 - by], order_send.at[at], order_recv.at[2 - by], at_clu(by))
        copy.start()
        order_copies.append(copy)

    def send_raw(i):
        group = [
            remote(own_columns(i), raw.at[i, core], raw_send.at[i, 0], raw_recv.at[i, core], at_clu(2)),
            remote(own_columns(i), raw.at[i, 4 + core], raw_send.at[i, 1], raw_recv.at[i, 4 + core], at_clu(-2)),
            remote(own_columns(i), raw.at[i, 2 + core], raw_send.at[i, 2], raw_recv.at[i, 2 + core], mate),
        ]
        for copy in group:
            copy.start()
            sends.append(copy)

    def arrived(i, slot):
        remote(raw.at[i, slot], raw.at[i, slot], raw_send.at[i, 0], raw_recv.at[i, slot], mate).wait_recv()

    def take_raw(i):
        for at, slot in ((3, core), (4, 4 + core)):
            arrived(i, slot)
            copy = remote(raw.at[i, slot], raw.at[i, slot], raw_send.at[i, at], raw_recv.at[i, slot], mate)
            copy.start()
            sends.append(copy)
        for slot in (3 - core, 1 - core, 5 - core):
            arrived(i, slot)

    send_raw(0)
    send_raw(1)

    lane = lax.broadcasted_iota(jnp.int32, (rank, coarse * rank), 1)
    row = lax.broadcasted_iota(jnp.int32, (rank, coarse * rank), 0)
    repeat = (lax.rem(lane, rank) == row).astype(BF16)
    wide = jnp.dot(coupling[...], repeat, preferred_element_type=F32)
    for b in range(far_count):
        start = targets[0, b] * rank
        keep = (lane >= start) & (lane < start + ranks[0, b])
        spread[b * rank:(b + 1) * rank, :] = jnp.where(keep, wide[b * rank:(b + 1) * rank, :], 0.0).astype(BF16)
    ext[quarter:, :] = jnp.zeros((ext.shape[0] - quarter, ext.shape[1]), BF16)

    sub = lax.broadcasted_iota(jnp.int32, (tile, tile), 0)
    lan = lax.broadcasted_iota(jnp.int32, (tile, tile), 1)
    upto = (sub <= lan).astype(BF16)
    first = (c - core - 2) * tile

    def ranked(chosen):
        spots = jnp.broadcast_to(chosen.astype(F32), (8, tile)).astype(BF16)
        return (jnp.dot(spots, upto, preferred_element_type=F32)[0:1, :] - 1.0).astype(jnp.int32)

    def one_hot(cluster_order, dst):
        spot = cluster_order - first
        spot = jnp.where(spot < 0, spot + n * tile, spot)
        spot = jnp.where(spot >= n * tile, spot - n * tile, spot)
        beyond = spot >= slots * tile
        spot = jnp.where(beyond, slots * tile + ranked(beyond), spot)
        down = jnp.broadcast_to(spot.astype(F32), (128, tile)).T
        at = lax.broadcasted_iota(jnp.int32, (tile, 128), 1).astype(F32)
        for j in range(dst.shape[1] // 128):
            dst[:, j * 128:(j + 1) * 128] = (down == at + float(j * 128)).astype(F32).astype(BF16)

    one_hot(order[...], own_pick)
    for copy in local:
        copy.wait()
    for at, by in enumerate(offsets):
        order_copies[at].wait_send()
        remote(orders.at[2 + by], orders.at[2 + by], order_send.at[at], order_recv.at[2 + by], mate).wait_recv()
    orders[2] = order[...]

    away = orders[1 + 2 * core] - c * tile
    chosen = (away >= 0) & (away < tile)
    place = jnp.where(chosen, ranked(chosen), -1)
    left = (lax.broadcasted_iota(jnp.int32, (ext.shape[0], tile), 0) == place).astype(F32).astype(BF16)
    right = (sub == away).astype(F32).astype(BF16)
    pick = lax.dot_general(left, right, (((1,), (1,)), ((), ())), preferred_element_type=F32).astype(BF16)
    for i in range(groups):
        block = jnp.concatenate([raw[i, 2 + core, d] for d in range(comps)], axis=1)
        got = jnp.dot(pick, block, preferred_element_type=F32).astype(BF16)
        ext_out[:, i * comps * width:(i + 1) * comps * width] = got[:quarter]
    ext_copy = remote(ext_out, ext.at[0:quarter], ext_send.at[0], ext_recv.at[0], at_clu(6 * core - 3))
    ext_copy.start()

    def gathered(pick_ref, i, with_ext):
        block = jnp.concatenate([raw[i, :, d].reshape(slots * tile, width) for d in range(comps)], axis=1)
        x = jnp.dot(pick_ref[:, :slots * tile], block, preferred_element_type=F32)
        if with_ext:
            x = x + jnp.dot(
                pick_ref[:, slots * tile:], ext[:, i * comps * width:(i + 1) * comps * width],
                preferred_element_type=F32,
            )
        x = x.astype(BF16)
        return jnp.concatenate([x[:, d * width:(d + 1) * width] for d in range(comps)], axis=0)

    take_raw(0)
    piece = jnp.dot(bases[...], gathered(own_pick, 0, False), preferred_element_type=F32)
    piece_out[...] = piece

    def piece_copy(d):
        return remote(piece_out, pieces.at[c], piece_send.at[d], piece_recv.at[c], at_clu(d))

    def start_piece(d, carry):
        piece_copy(d).start()
        return carry

    lax.fori_loop(1, n, start_piece, 0)
    pieces[c] = piece
    for i in range(2, groups):
        send_raw(i)

    for j in range(near_count):
        spot = near_col[0, j] - c + 2
        spot = jnp.where(spot < 0, spot + n, spot)
        spot = jnp.where(spot >= n, spot - n, spot)
        one_hot(orders[jnp.clip(spot, 0, 4)], picks.at[j])
    tiles_copy.wait()
    basis_copy.wait()

    def near(i):
        part = jnp.zeros((rows, width), F32)
        for j in range(near_count):
            part = part + jnp.dot(tiles[j], gathered(picks.at[j], i, True), preferred_element_type=F32)
        total[i] = part

    def send_y(i):
        y_out[i] = total[i].astype(BF16)
        copy = remote(y_out.at[i], y_in.at[i], y_send.at[i], y_recv.at[i], at_grp(i))
        copy.start()
        sends.append(copy)

    take_raw(1)
    ext_copy.wait_recv()
    near(1)

    def await_piece(d, carry):
        source = lax.rem(c + d, n)
        remote(piece_out, pieces.at[source], piece_send.at[d], piece_recv.at[source], at_clu(d)).wait_recv()
        return carry

    lax.fori_loop(1, n, await_piece, 0)
    for level in range(levels):
        count = 2 ** (level + 1)
        members = n // count
        for k in range(count):
            entry = lax.fori_loop(
                0, members,
                lambda m, acc, k=k, members=members, level=level: acc
                + pieces[k * members + m, level * rank:(level + 1) * rank, :],
                jnp.zeros((rank, width), F32),
            )
            at = (count - 2 + k) * rank
            table_out[at:at + rank, :] = entry
            tables[0, at:at + rank, :] = entry
    for d in range(1, groups):
        copy = remote(table_out, tables.at[groups - d], table_send.at[d], table_recv.at[groups - d], at_grp(d))
        copy.start()
        sends.append(copy)
    near(0)
    for i in range(2, groups - 1):
        take_raw(i)
        near(i)

    for d in range(1, groups):
        remote(table_out, tables.at[d], table_send.at[d], table_recv.at[d], at_grp(d)).wait_recv()
    table = jnp.concatenate([tables[i] for i in range(groups)], axis=1)
    high = table.astype(BF16)
    low = (table - high.astype(F32)).astype(BF16)
    mixed = jnp.dot(spread[...], high, preferred_element_type=F32)
    mixed = mixed + jnp.dot(spread[...], low, preferred_element_type=F32)
    for b in range(far_count):
        coupled[b * rank:(b + 1) * rank, :] = (mixed[b * rank:(b + 1) * rank, :] * scale[0, b]).astype(BF16)
    far = lax.dot_general(basis[...], coupled[...], (((0,), (0,)), ((), ())), preferred_element_type=F32)
    for i in range(groups - 1):
        total[i] = total[i] + far[:, i * width:(i + 1) * width]
    total[groups - 1] = far[:, (groups - 1) * width:]
    for i in range(1, groups - 1):
        send_y(i)
    last = groups - 1
    far_part = total[last]
    take_raw(last)
    near(last)
    total[last] = total[last] + far_part
    send_y(last)

    answer = total[0]
    for i in range(1, groups):
        remote(y_out.at[i], y_in.at[i], y_send.at[i], y_recv.at[i], at_grp(i)).wait_recv()
        answer = answer + y_in[i].astype(F32)
    out[...] = answer.reshape(comps, tile, width)

    for copy in sends:
        copy.wait_send()
    ext_copy.wait_send()

    def end_piece(d, carry):
        piece_copy(d).wait_send()
        return carry

    lax.fori_loop(1, n, end_piece, 0)


def solution(mesh):
    n, groups = mesh.shape["clu"], mesh.shape["grp"]

    def on_device(forces, order, bases, near_tiles, near_col, far_basis, far_coupling, far_scale, far_rank, far_target):
        comps, tile, columns = forces.shape
        levels, rank = bases.shape[:2]
        near_count, far_count = near_tiles.shape[1], far_basis.shape[1]
        width, rows, quarter = columns // groups, comps * tile, tile // 4
        coarse = 2 ** (levels + 1) - 2
        slots = 6
        pad = 128
        vmem, smem, hbm = (pl.BlockSpec(memory_space=m) for m in (pltpu.VMEM, pltpu.SMEM, pl.ANY))
        dma = pltpu.SemaphoreType.DMA
        return pl.pallas_call(
            functools.partial(kernel, n, groups, levels, rank),
            out_shape=jax.ShapeDtypeStruct((comps, tile, width), F32),
            in_specs=[hbm, vmem, vmem, hbm, smem, hbm, vmem, smem, smem, smem],
            out_specs=vmem,
            scratch_shapes=[
                pltpu.VMEM((groups, slots, comps, tile, width), BF16),
                pltpu.VMEM((pad, comps * columns), BF16),
                pltpu.VMEM((quarter, comps * columns), BF16),
                pltpu.VMEM((5, 1, tile), jnp.int32),
                pltpu.VMEM((near_count, rows, rows), BF16),
                pltpu.VMEM((far_count * rank, rows), BF16),
                pltpu.VMEM((far_count * rank, coarse * rank), BF16),
                pltpu.VMEM((near_count, tile, slots * tile + pad), BF16),
                pltpu.VMEM((tile, slots * tile), BF16),
                pltpu.VMEM((levels * rank, width), F32),
                pltpu.VMEM((n, levels * rank, width), F32),
                pltpu.VMEM((coarse * rank, width), F32),
                pltpu.VMEM((groups, coarse * rank, width), F32),
                pltpu.VMEM((far_count * rank, columns), BF16),
                pltpu.VMEM((groups, rows, width), F32),
                pltpu.VMEM((groups, rows, width), BF16),
                pltpu.VMEM((groups, rows, width), BF16),
                dma((groups + 2,)),
                dma((4,)), dma((5,)),
                dma((groups, 5)), dma((groups, slots)),
                dma((1,)), dma((1,)),
                dma((n,)), dma((n,)),
                dma((groups,)), dma((groups,)),
                dma((groups,)), dma((groups,)),
            ],
            compiler_params=pltpu.CompilerParams(
                collective_id=0, has_side_effects=True, vmem_limit_bytes=60 * 1024 * 1024
            ),
        )(
            forces,
            order.reshape(1, tile),
            bases.reshape(levels * rank, rows),
            near_tiles.reshape(near_count, rows, rows),
            near_col,
            far_basis.reshape(far_count * rank, rows),
            far_coupling.reshape(far_count * rank, rank),
            far_scale,
            far_rank,
            far_target,
        )

    placed = (
        P(None, "clu", None),
        P("clu"),
        P(None, None, None, "clu"),
        P("clu", "grp", None, None),
        P("clu", "grp"),
        P("clu", "grp", None, None),
        P("clu", "grp", None, None),
        P("clu", "grp"),
        P("clu", "grp"),
        P("clu", "grp"),
    )
    return jax.shard_map(
        on_device, mesh=mesh, in_specs=placed, out_specs=P(None, "clu", "grp"), check_vma=False
    )
```

```python
import functools

import jax
import jax.numpy as jnp
from jax import lax
from jax.experimental import pallas as pl
from jax.experimental.pallas import tpu as pltpu
from jax.sharding import PartitionSpec as P

MESH = pl.DeviceIdType.MESH
F32, BF16 = jnp.float32, jnp.bfloat16


def kernel(
    n, groups, levels, rank,
    forces, order, bases, tiles_hbm, near_col, basis_hbm, coupling, scale, ranks, targets,
    out,
    raw, ext, ext_out, orders, tiles, basis, spread, picks, own_pick, piece_out, piece_mate, pieces,
    table_out, tables, coupled, total, y_out, y_in,
    local_sem, order_send, order_recv, raw_send, raw_recv, ext_send, ext_recv,
    piece_send, piece_recv, table_send, table_recv, y_send, y_recv,
):
    g, c = lax.axis_index("grp"), lax.axis_index("clu")
    core = lax.rem(c, 2)
    comps, tile, columns = forces.shape
    width = columns // groups
    quarter = tile // 4
    slots = raw.shape[1]
    rows = comps * tile
    near_count = tiles.shape[0]
    far_count = targets.shape[1]
    coarse = 2 ** (levels + 1) - 2
    half = n // 2

    def at_clu(by):
        return {"grp": g, "clu": lax.rem(c + by + n, n)}

    partners = (g, g + 1 - 2 * lax.rem(g, 2), lax.rem(g + 2, groups), groups - 1 - g)

    def at_grp(i):
        return {"grp": partners[i], "clu": c}

    mate = {"grp": g, "clu": c + 1 - 2 * core}

    def remote(src, dst, send, recv, where):
        return pltpu.make_async_remote_copy(
            src_ref=src, dst_ref=dst, send_sem=send, recv_sem=recv, device_id=where, device_id_type=MESH
        )

    def own_columns(i):
        q = partners[i]
        return forces.at[:, :, pl.ds(pl.multiple_of(q * width, width), width)]

    local = [pltpu.make_async_copy(own_columns(i), raw.at[i, 2 + core], local_sem.at[i]) for i in range(groups)]
    for copy in local:
        copy.start()
    tiles_copy = pltpu.make_async_copy(tiles_hbm, tiles, local_sem.at[groups])
    basis_copy = pltpu.make_async_copy(basis_hbm, basis, local_sem.at[groups + 1])
    tiles_copy.start()
    basis_copy.start()

    barrier = pltpu.get_barrier_semaphore()

    def greet(d, carry):
        pl.semaphore_signal(barrier, inc=1, device_id=at_clu(d), device_id_type=MESH)
        return carry

    lax.fori_loop(1, n, greet, 0)
    for d in range(1, groups):
        pl.semaphore_signal(barrier, inc=1, device_id=at_grp(d), device_id_type=MESH)
    pl.semaphore_wait(barrier, n - 1 + groups - 1)

    sends = []
    near_groups, far_group = range(1, groups - 1), groups - 1
    offsets = (-2, -1, 1, 2)
    order_copies = []
    for at, by in enumerate(offsets):
        copy = remote(order, orders.at[2 - by], order_send.at[at], order_recv.at[2 - by], at_clu(by))
        copy.start()
        order_copies.append(copy)

    def send_raw(i):
        group = [
            remote(own_columns(i), raw.at[i, core], raw_send.at[i, 0], raw_recv.at[i, core], at_clu(2)),
            remote(own_columns(i), raw.at[i, 4 + core], raw_send.at[i, 1], raw_recv.at[i, 4 + core], at_clu(-2)),
        ]
        for copy in group:
            copy.start()
            sends.append(copy)

    def send_mate(i):
        copy = remote(own_columns(i), raw.at[i, 2 + core], raw_send.at[i, 2], raw_recv.at[i, 2 + core], mate)
        copy.start()
        sends.append(copy)

    def arrived(i, slot):
        remote(raw.at[i, slot], raw.at[i, slot], raw_send.at[i, 0], raw_recv.at[i, slot], mate).wait_recv()

    def take_raw(i):
        for at, slot in ((3, core), (4, 4 + core)):
            arrived(i, slot)
            if i == 0:
                for to in near_groups:
                    across = remote(
                        raw.at[0, slot], raw.at[to, slot], raw_send.at[to, at - 3], raw_recv.at[to, slot], at_grp(to)
                    )
                    across.start()
                    sends.append(across)
            copy = remote(raw.at[i, slot], raw.at[i, slot], raw_send.at[i, at], raw_recv.at[i, slot], mate)
            copy.start()
            sends.append(copy)
        for slot in (3 - core, 1 - core, 5 - core):
            arrived(i, slot)

    send_raw(0)
    for i in range(groups):
        send_mate(i)

    lane = lax.broadcasted_iota(jnp.int32, (rank, coarse * rank), 1)
    row = lax.broadcasted_iota(jnp.int32, (rank, coarse * rank), 0)
    repeat = (lax.rem(lane, rank) == row).astype(BF16)
    wide = jnp.dot(coupling[...], repeat, preferred_element_type=F32)
    for b in range(far_count):
        start = targets[0, b] * rank
        keep = (lane >= start) & (lane < start + ranks[0, b])
        spread[b * rank:(b + 1) * rank, :] = jnp.where(keep, wide[b * rank:(b + 1) * rank, :], 0.0).astype(BF16)
    ext[:, quarter:, :] = jnp.zeros((groups, ext.shape[1] - quarter, ext.shape[2]), BF16)

    sub = lax.broadcasted_iota(jnp.int32, (tile, tile), 0)
    lan = lax.broadcasted_iota(jnp.int32, (tile, tile), 1)
    upto = (sub <= lan).astype(BF16)
    first = (c - core - 2) * tile

    def ranked(chosen):
        spots = jnp.broadcast_to(chosen.astype(F32), (8, tile)).astype(BF16)
        return (jnp.dot(spots, upto, preferred_element_type=F32)[0:1, :] - 1.0).astype(jnp.int32)

    def one_hot(cluster_order, dst):
        spot = cluster_order - first
        spot = jnp.where(spot < 0, spot + n * tile, spot)
        spot = jnp.where(spot >= n * tile, spot - n * tile, spot)
        beyond = spot >= slots * tile
        spot = jnp.where(beyond, slots * tile + ranked(beyond), spot)
        down = jnp.broadcast_to(spot.astype(F32), (128, tile)).T
        at = lax.broadcasted_iota(jnp.int32, (tile, 128), 1).astype(F32)
        for j in range(dst.shape[1] // 128):
            dst[:, j * 128:(j + 1) * 128] = (down == at + float(j * 128)).astype(F32).astype(BF16)

    one_hot(order[...], own_pick)
    for copy in local:
        copy.wait()
    for at, by in enumerate(offsets):
        order_copies[at].wait_send()
        remote(orders.at[2 + by], orders.at[2 + by], order_send.at[at], order_recv.at[2 + by], mate).wait_recv()
    orders[2] = order[...]

    away = orders[1 + 2 * core] - c * tile
    chosen = (away >= 0) & (away < tile)
    place = jnp.where(chosen, ranked(chosen), -1)
    left = (lax.broadcasted_iota(jnp.int32, (ext.shape[1], tile), 0) == place).astype(F32).astype(BF16)
    right = (sub == away).astype(F32).astype(BF16)
    pick = lax.dot_general(left, right, (((1,), (1,)), ((), ())), preferred_element_type=F32).astype(BF16)
    for at, i in enumerate((0, far_group)):
        block = jnp.concatenate([raw[i, 2 + core, d] for d in range(comps)], axis=1)
        ext_out[at] = jnp.dot(pick, block, preferred_element_type=F32).astype(BF16)[:quarter]
        copy = remote(
            ext_out.at[at], ext.at[i, 0:quarter], ext_send.at[i], ext_recv.at[i], at_clu(6 * core - 3)
        )
        copy.start()
        sends.append(copy)

    def take_ext(i):
        rows_in = ext.at[i, 0:quarter]
        remote(rows_in, rows_in, ext_send.at[i], ext_recv.at[i], mate).wait_recv()

    def gathered(pick_ref, i, with_ext):
        block = jnp.concatenate([raw[i, :, d].reshape(slots * tile, width) for d in range(comps)], axis=1)
        x = jnp.dot(pick_ref[:, :slots * tile], block, preferred_element_type=F32)
        if with_ext:
            x = x + jnp.dot(
                pick_ref[:, slots * tile:], ext[i], preferred_element_type=F32
            )
        x = x.astype(BF16)
        return jnp.concatenate([x[:, d * width:(d + 1) * width] for d in range(comps)], axis=0)

    take_raw(0)
    own_rows = gathered(own_pick, 0, False)
    piece = jnp.zeros((levels * rank, width), F32)
    for d in range(comps):
        part = jnp.concatenate([bases[level, d] for level in range(levels)], axis=0)
        piece = piece + jnp.dot(part, own_rows[d * tile:(d + 1) * tile], preferred_element_type=F32)
    piece_out[0] = piece
    copy = remote(piece_out.at[0], piece_mate, piece_send.at[0], piece_recv.at[half], mate)
    copy.start()
    sends.append(copy)
    copy.wait_recv()
    pair = piece + piece_mate[...]
    piece_out[1] = pair
    pieces[c // 2] = pair

    def piece_copy(d):
        return remote(piece_out.at[1], pieces.at[c // 2], piece_send.at[d], piece_recv.at[c // 2], at_clu(2 * d))

    def start_piece(d, carry):
        piece_copy(d).start()
        return carry

    lax.fori_loop(1, half, start_piece, 0)
    send_raw(far_group)

    for j in range(near_count):
        spot = near_col[0, j] - c + 2
        spot = jnp.where(spot < 0, spot + n, spot)
        spot = jnp.where(spot >= n, spot - n, spot)
        one_hot(orders[jnp.clip(spot, 0, 4)], picks.at[j])
    tiles_copy.wait()
    basis_copy.wait()

    def near(i):
        part = jnp.zeros((rows, width), F32)
        for j in range(near_count):
            part = part + jnp.dot(tiles[j], gathered(picks.at[j], i, True), preferred_element_type=F32)
        total[i] = part

    def send_y(i):
        y_out[i] = total[i].astype(BF16)
        copy = remote(y_out.at[i], y_in.at[i], y_send.at[i], y_recv.at[i], at_grp(i))
        copy.start()
        sends.append(copy)

    take_ext(0)
    for to in near_groups:
        across = remote(
            ext.at[0, 0:quarter], ext.at[to, 0:quarter], ext_send.at[to], ext_recv.at[to], at_grp(to)
        )
        across.start()
        sends.append(across)

    def await_piece(d, carry):
        source = lax.rem(c // 2 + d, half)
        remote(piece_out.at[1], pieces.at[source], piece_send.at[d], piece_recv.at[source], mate).wait_recv()
        return carry

    lax.fori_loop(1, half, await_piece, 0)
    for level in range(levels):
        count = 2 ** (level + 1)
        members = half // count
        for k in range(count):
            entry = lax.fori_loop(
                0, members,
                lambda m, acc, k=k, members=members, level=level: acc
                + pieces[k * members + m, level * rank:(level + 1) * rank, :],
                jnp.zeros((rank, width), F32),
            )
            at = (count - 2 + k) * rank
            table_out[at:at + rank, :] = entry
            tables[0, at:at + rank, :] = entry
    for d in range(1, groups):
        copy = remote(table_out, tables.at[d], table_send.at[d], table_recv.at[d], at_grp(d))
        copy.start()
        sends.append(copy)
    near(0)
    for i in near_groups:
        take_raw(i)
        take_ext(i)
        near(i)

    for d in range(1, groups):
        remote(table_out, tables.at[d], table_send.at[d], table_recv.at[d], at_grp(d)).wait_recv()
    table = jnp.concatenate([tables[i] for i in range(groups)], axis=1)
    high = table.astype(BF16)
    low = (table - high.astype(F32)).astype(BF16)
    mixed = jnp.dot(spread[...], high, preferred_element_type=F32)
    mixed = mixed + jnp.dot(spread[...], low, preferred_element_type=F32)
    for b in range(far_count):
        coupled[b * rank:(b + 1) * rank, :] = (mixed[b * rank:(b + 1) * rank, :] * scale[0, b]).astype(BF16)
    far = lax.dot_general(basis[...], coupled[...], (((0,), (0,)), ((), ())), preferred_element_type=F32)
    for i in range(groups - 1):
        total[i] = total[i] + far[:, i * width:(i + 1) * width]
    total[groups - 1] = far[:, (groups - 1) * width:]
    for i in range(1, groups - 1):
        send_y(i)
    last = groups - 1
    far_part = total[last]
    take_raw(last)
    take_ext(last)
    near(last)
    total[last] = total[last] + far_part
    send_y(last)

    answer = total[0]
    for i in range(1, groups):
        remote(y_out.at[i], y_in.at[i], y_send.at[i], y_recv.at[i], at_grp(i)).wait_recv()
        answer = answer + y_in[i].astype(F32)
    out[...] = answer.reshape(comps, tile, width)

    for copy in sends:
        copy.wait_send()

    def end_piece(d, carry):
        piece_copy(d).wait_send()
        return carry

    lax.fori_loop(1, half, end_piece, 0)


def solution(mesh):
    n, groups = mesh.shape["clu"], mesh.shape["grp"]

    def on_device(forces, order, bases, near_tiles, near_col, far_basis, far_coupling, far_scale, far_rank, far_target):
        comps, tile, columns = forces.shape
        levels, rank = bases.shape[:2]
        near_count, far_count = near_tiles.shape[1], far_basis.shape[1]
        width, rows, quarter = columns // groups, comps * tile, tile // 4
        coarse = 2 ** (levels + 1) - 2
        slots = 6
        pad = 128
        vmem, smem, hbm = (pl.BlockSpec(memory_space=m) for m in (pltpu.VMEM, pltpu.SMEM, pl.ANY))
        dma = pltpu.SemaphoreType.DMA
        return pl.pallas_call(
            functools.partial(kernel, n, groups, levels, rank),
            out_shape=jax.ShapeDtypeStruct((comps, tile, width), F32),
            in_specs=[hbm, vmem, vmem, hbm, smem, hbm, vmem, smem, smem, smem],
            out_specs=vmem,
            scratch_shapes=[
                pltpu.VMEM((groups, slots, comps, tile, width), BF16),
                pltpu.VMEM((groups, pad, comps * width), BF16),
                pltpu.VMEM((2, quarter, comps * width), BF16),
                pltpu.VMEM((5, 1, tile), jnp.int32),
                pltpu.VMEM((near_count, rows, rows), BF16),
                pltpu.VMEM((far_count * rank, rows), BF16),
                pltpu.VMEM((far_count * rank, coarse * rank), BF16),
                pltpu.VMEM((near_count, tile, slots * tile + pad), BF16),
                pltpu.VMEM((tile, slots * tile), BF16),
                pltpu.VMEM((2, levels * rank, width), F32),
                pltpu.VMEM((levels * rank, width), F32),
                pltpu.VMEM((n // 2, levels * rank, width), F32),
                pltpu.VMEM((coarse * rank, width), F32),
                pltpu.VMEM((groups, coarse * rank, width), F32),
                pltpu.VMEM((far_count * rank, columns), BF16),
                pltpu.VMEM((groups, rows, width), F32),
                pltpu.VMEM((groups, rows, width), BF16),
                pltpu.VMEM((groups, rows, width), BF16),
                dma((groups + 2,)),
                dma((4,)), dma((5,)),
                dma((groups, 5)), dma((groups, slots)),
                dma((groups,)), dma((groups,)),
                dma((n // 2,)), dma((n // 2 + 1,)),
                dma((groups,)), dma((groups,)),
                dma((groups,)), dma((groups,)),
            ],
            compiler_params=pltpu.CompilerParams(
                collective_id=0, has_side_effects=True, vmem_limit_bytes=60 * 1024 * 1024
            ),
        )(
            forces,
            order.reshape(1, tile),
            jnp.transpose(bases, (0, 2, 1, 3)),
            near_tiles.reshape(near_count, rows, rows),
            near_col,
            far_basis.reshape(far_count * rank, rows),
            far_coupling.reshape(far_count * rank, rank),
            far_scale,
            far_rank,
            far_target,
        )

    placed = (
        P(None, "clu", None),
        P("clu"),
        P(None, None, None, "clu"),
        P("clu", "grp", None, None),
        P("clu", "grp"),
        P("clu", "grp", None, None),
        P("clu", "grp", None, None),
        P("clu", "grp"),
        P("clu", "grp"),
        P("clu", "grp"),
    )
    return jax.shard_map(
        on_device, mesh=mesh, in_specs=placed, out_specs=P(None, "clu", "grp"), check_vma=False
    )
```
